512 devices in a mesh: psg: 128 (over z, x, core), head: 4 (over y).
Axes of the slice: x: 4, y: 4, z: 16, core: 2. Of those that a mesh axis runs over, the one named last changes fastest.
Arguments:
- queries: bfloat16 [1024, 2048], P('psg', 'head'), may hold values from -16 to 16
- passage_keys: bfloat16 [256, 256, 2048], P('psg', None, 'head'), may hold values from -6 to 6
- passage_values: bfloat16 [256, 256, 2048], P('psg', None, 'head'), may hold values from -6 to 6
- shelf_ids: int32 [1024, 16], P('psg'), may hold values from 0 to 127, all different within a row; in each aligned block of 8 rows (0 to 7, 8 to 15, ...) at most 2 rows name the same one
- live_mask: int32 [1024, 32], P('psg'), may hold values 0 or 1
- w_out: bfloat16 [2048, 2048], P('head'), may hold values from -0.75 to 0.75
Outputs:
- out: bfloat16 [1024, 2048], P('psg', 'head')
The draws below stay inside these ranges and needn't reach their ends.
Inputs may be any that keep to these rules, and one draw needn't show every extreme that they name: `shelf_ids`: each row names 16 different shelves. Among the rows of one device, no shelf is named by more than 2 rows, and in some devices one shelf is named by exactly 2 rows.
All inputs are finite; a program needn't handle non-finite values. No bound on the sum of `live_mask` on one device may be relied on, other than what follows from the above.
Results may differ from the reference program's by a relative error of at most 0.0085.
Values may be sent and summed in bfloat16 or wider, within the bound.
No kernel may reach another device: no remote copies, remote signals or barrier semaphores. Data moves between devices by JAX's collectives and lax.ppermute only.
A program may use at most 64 MiB of HBM per device.

```python
import math
import jax
import jax.numpy as jnp
import numpy as np
from jax import lax

D = 2048
H = 32
DK = 64
LEN = 256
PSG_DEV = 2
REQ_DEV = 8
SHELVES = 16
MOST = 2
HD = 2048
PASSAGES = 256
REQUESTS = 1024
ENTRIES = 32
N_PSG = 128


def draw_passage_keys(key, part):
    drawn = jnp.clip(jax.random.normal(jax.random.fold_in(key, 1), (PASSAGES, LEN, HD), jnp.float32), -5.0, 5.0)
    return drawn.astype(jnp.bfloat16)


def draw_queries(key, part):
    drawn = jnp.clip(jax.random.normal(jax.random.fold_in(key, 3), (REQUESTS, HD), jnp.float32), -5.0, 5.0) * 0.3
    return drawn.astype(jnp.bfloat16)


def place_ends(entries, key, low, top_value):
    longest = entries.shape.index(max(entries.shape))
    spots = []
    for shift in (0, 1):
        where = [jax.random.randint(jax.random.fold_in(key, axis), (), 0, length) for axis, length in enumerate(entries.shape)]
        where[longest] = (where[longest] + shift) % entries.shape[longest]
        spots.append(tuple(where))
    return entries.at[spots[0]].set(low).at[spots[1]].set(top_value)


def level_of(own_key, extent, cuts, smallest, largest):
    factor_of, own = 1.0, jax.random.fold_in(own_key, 6)
    for dim, shards_of in cuts:
        heights = jnp.exp(jax.random.uniform(jax.random.fold_in(own, dim), (shards_of,), jnp.float32, smallest / len(cuts), largest / len(cuts)))
        factor_of = factor_of * jnp.repeat(heights, extent[dim] // shards_of).reshape([-1 if axis == dim else 1 for axis in range(len(extent))])
    return factor_of


def assign_block(stream_key, own, number, rows, amount, top, limit, lean):
    order = jax.random.permutation(stream_key, amount)
    crowded, ordinary = shares(amount, rows * top, limit, lean, True), shares(amount, rows * top, limit, lean, False)
    places = jnp.arange(amount)

    def named(tallies, offset_by):
        used = int((tallies > 0).sum())
        fixed = max(1, used // 4)
        shifted = fixed + (places - fixed + offset_by * (used - fixed)) % max(1, amount - fixed)
        return jnp.zeros((amount,), jnp.int32).at[order[jnp.where(places < fixed, places, shifted)]].set(jnp.asarray(tallies, jnp.int32))

    tallies = jnp.where(number % 4 == 0, named(crowded, number // 4), named(ordinary, number - number // 4 - 1))
    mixed = jax.random.permutation(jax.random.fold_in(own, 3), amount)
    source_of, sink = mixed[0:amount // 2 * 2:2], mixed[1:amount // 2 * 2:2]
    slack = jnp.minimum(tallies[source_of] - 1, limit - tallies[sink]) // 2
    slack = jnp.where((source_of == order[0]) | (sink == order[0]) | (tallies[sink] == 0), 0, jnp.maximum(slack, 0))
    shifted = jax.random.randint(jax.random.fold_in(own, 4), (amount // 2,), 0, 1 << 20) % (slack + 1)
    tallies = tallies.at[source_of].add(-shifted).at[sink].add(shifted)
    members = jnp.searchsorted(jnp.cumsum(tallies), jnp.arange(rows * top), side="right").astype(jnp.int32)
    listing = members.reshape(top, rows).T
    listing = listing[jax.random.permutation(jax.random.fold_in(own, 1), rows)]
    offset_by = jax.random.randint(jax.random.fold_in(own, 2), (rows, 1), 0, top)
    return jnp.take_along_axis(listing, (jnp.arange(top)[None, :] + offset_by) % top, axis=1)


def shares(amount, total, reach, lean, full):
    loads = [(1 << 20) // math.isqrt(standing ** lean) + 1 for standing in range(1, amount + 1)]
    largest = reach if full else min(reach, max(-(-total // amount), total * loads[0] // sum(loads)))
    least = 1 if total - largest >= amount - 1 else 0
    counts, surplus = [largest] + [least] * (amount - 1), total - largest - least * (amount - 1)
    while surplus > 0:
        free = [i for i in range(1, amount) if counts[i] < largest] or [i for i in range(1, amount) if counts[i] < reach]
        mass, budget = sum([loads[i] for i in free]), surplus
        for i in free:
            more = min(reach - counts[i], max(1, budget * loads[i] // mass), surplus)
            counts[i] = counts[i] + more
            surplus = surplus - more
    return np.array(counts)


def gaussian(own_key, shape, width, most, shards=(), kind=jnp.bfloat16):
    values = jax.random.normal(own_key, shape, jnp.float32) * width
    if len(shards) > 0:
        values = level_of(own_key, shape, shards, -0.22, 0.18) * values
    return jnp.clip(values, min=-most, max=most).astype(kind)


def setup_inputs(seed: int = 0) -> dict:
    keys = jax.random.split(jax.random.key(seed), 7)
    queries = draw_queries(jax.random.fold_in(keys[6], 71), 0)
    passage_keys = draw_passage_keys(jax.random.fold_in(keys[6], 71), 0)
    passage_values = gaussian(keys[2], (PASSAGES, LEN, HD), 1.0, 6.0, ((0, 128), (2, 4)))
    shelf_ids_keys = jax.random.split(jax.random.fold_in(keys[3], 1), REQUESTS // REQ_DEV)
    shelf_ids_turns = jax.random.permutation(jax.random.fold_in(keys[3], 3), REQUESTS // REQ_DEV)
    shelf_ids = jax.vmap(lambda own, number: assign_block(jax.random.fold_in(keys[3], 2), own, number, REQ_DEV, N_PSG, SHELVES, MOST, 1))(shelf_ids_keys, shelf_ids_turns).reshape((REQUESTS, SHELVES))
    live_mask = place_ends((jax.random.randint(keys[4], (REQUESTS, ENTRIES), 0, 4) < 3).astype(jnp.int32), jax.random.fold_in(keys[4], 1), 0, 1)
    w_out = gaussian(keys[5], (HD, D), (HD // 32) ** -0.5, 0.75, ((0, 4),))
    return dict(queries=queries, passage_keys=passage_keys, passage_values=passage_values, shelf_ids=shelf_ids, live_mask=live_mask, w_out=w_out)


far_below = -1e+30

def shelf_partials(query_rows, live_bits, passage_keys, passage_values):
    row_count = query_rows.shape[0]
    heads_here = query_rows.shape[1] // DK
    passages_here = passage_keys.shape[0]
    length = passage_keys.shape[1]
    query_heads = query_rows.astype(jnp.float32).reshape(row_count, heads_here, DK).transpose(1, 0, 2)
    key_heads = passage_keys.astype(jnp.float32).reshape(passages_here * length, heads_here, DK).transpose(1, 0, 2)
    value_heads = passage_values.astype(jnp.float32).reshape(passages_here * length, heads_here, DK).transpose(1, 0, 2)
    key_live = jnp.repeat(live_bits > 0, length, axis=1)

    def one_head(operands):
        query_head, key_head, value_head = operands
        scores = jnp.dot(query_head, key_head.T)
        scores = jnp.where(key_live, scores, far_below)
        peak_score = jnp.max(scores, axis=1)
        exp_scores = jnp.exp(scores - peak_score[:, None])
        exp_total = jnp.sum(exp_scores, axis=1)
        weights = exp_scores.astype(jnp.bfloat16).astype(jnp.float32)
        context = jnp.dot(weights, value_head) / exp_total[:, None]
        return (context, peak_score, exp_total)
    context, peak_score, exp_total = lax.map(one_head, (query_heads, key_heads, value_heads))
    return (context.transpose(1, 0, 2).reshape(row_count, heads_here * DK), peak_score.T, exp_total.T)

def merge_shelves(context, peak_score, exp_total, has_live):
    request_count, shelf_count, heads_here = peak_score.shape
    masked_peak = jnp.where(has_live[:, :, None], peak_score, far_below)
    best_peak = jnp.max(masked_peak, axis=1)
    shelf_share = jnp.where(has_live[:, :, None], exp_total * jnp.exp(masked_peak - best_peak[:, None, :]), 0.0)
    context_heads = context.reshape(request_count, shelf_count, heads_here, DK)
    attended = jnp.sum(shelf_share[:, :, :, None] * context_heads, axis=1) / jnp.sum(shelf_share, axis=1)[:, :, None]
    return attended.reshape(request_count, heads_here * DK).astype(jnp.bfloat16)

def reference(queries, passage_keys, passage_values, shelf_ids, live_mask, w_out):
    first_entry = (jnp.arange(ENTRIES, dtype=jnp.int32) == 0).astype(jnp.int32)
    live_bits = jnp.maximum(live_mask, first_entry[None, :]).reshape(REQUESTS, SHELVES, PSG_DEV)
    owner_ids = jnp.arange(N_PSG, dtype=jnp.int32)
    presence = jnp.sum((shelf_ids[:, :, None] == owner_ids[None, None, :]).astype(jnp.int32), axis=1)
    blocks = presence.reshape(N_PSG, REQ_DEV, N_PSG)
    rank_table = (jnp.cumsum(blocks, axis=1) - blocks).reshape(REQUESTS, N_PSG).astype(jnp.int32)
    slot_index = jnp.take_along_axis(rank_table, shelf_ids, axis=1).astype(jnp.int32)
    source = (jnp.arange(REQUESTS, dtype=jnp.int32) // REQ_DEV)[:, None]
    box_index = ((shelf_ids * N_PSG + source) * MOST + slot_index).reshape(-1).astype(jnp.int32)
    row_ids = jnp.broadcast_to(jnp.arange(REQUESTS, dtype=jnp.int32)[:, None], (REQUESTS, SHELVES)).reshape(-1)
    box_rows = N_PSG * MOST
    slot_table = jnp.full((N_PSG * box_rows,), REQUESTS, jnp.int32).at[box_index].set(row_ids)
    live_table = jnp.zeros((N_PSG * box_rows, PSG_DEV), jnp.int32).at[box_index].set(live_bits.reshape(-1, PSG_DEV))
    padded = jnp.concatenate([queries, jnp.zeros((1, HD), jnp.bfloat16)], axis=0)

    def owner_work(owner_index):
        start = (owner_index * box_rows).astype(jnp.int32)
        rows = lax.dynamic_slice_in_dim(slot_table, start, box_rows)
        owner_live = lax.dynamic_slice_in_dim(live_table, start, box_rows, 0)
        first_passage = (owner_index * PSG_DEV).astype(jnp.int32)
        owner_keys = lax.dynamic_slice_in_dim(passage_keys, first_passage, PSG_DEV, 0)
        owner_values = lax.dynamic_slice_in_dim(passage_values, first_passage, PSG_DEV, 0)
        return shelf_partials(padded[rows], owner_live, owner_keys, owner_values)
    context, peak_score, exp_total = lax.map(owner_work, owner_ids)
    context = context.reshape(N_PSG * box_rows, HD)[box_index].reshape(REQUESTS, SHELVES, HD)
    peak_score = peak_score.reshape(N_PSG * box_rows, H)[box_index].reshape(REQUESTS, SHELVES, H)
    exp_total = exp_total.reshape(N_PSG * box_rows, H)[box_index].reshape(REQUESTS, SHELVES, H)
    has_live = jnp.max(live_bits, axis=2) > 0
    attended = merge_shelves(context, peak_score, exp_total, has_live)
    return jnp.dot(attended.astype(jnp.float32), w_out.astype(jnp.float32), preferred_element_type=jnp.float32).astype(jnp.bfloat16)
```

```python
import jax
import jax.numpy as jnp
from jax import lax
from jax.experimental import pallas as pl
from jax.experimental.pallas import tpu as pltpu
from jax.sharding import PartitionSpec as P

DK = 64
SLOTS = 2
LANES = 128
far_below = -1e30
bf16 = jnp.bfloat16
f32 = jnp.float32


def first_member(owners):
    return owners // 2 + owners // 32 + 1 if owners >= 32 else 0


def rotated_group(owners):
    first = first_member(owners)
    return [[(first + i) % owners for i in range(owners)]]


def dot(a, b, dims):
    return lax.dot_general(a, b, (dims, ((), ())), preferred_element_type=f32)


def choose(shelf_ids, live_mask, owners):
    requests, shelves = shelf_ids.shape
    columns = owners * SLOTS
    column = lax.broadcasted_iota(jnp.int32, (requests, columns), 1)
    position = column // SLOTS + first_member(owners)
    owner = jnp.where(position >= owners, position - owners, position)
    present = jnp.zeros((requests, columns), f32)
    live0 = jnp.zeros((requests, columns), f32)
    live1 = jnp.zeros((requests, columns), f32)
    for j in range(shelves):
        hit = (shelf_ids[:, j : j + 1] == owner).astype(f32)
        present = present + hit
        first = live_mask[:, 2 * j : 2 * j + 1].astype(f32)
        first = jnp.ones_like(first) if j == 0 else first
        live0 = live0 + hit * first
        live1 = live1 + hit * live_mask[:, 2 * j + 1 : 2 * j + 2].astype(f32)
    rank = jnp.zeros((1, columns), f32)
    ranks = []
    for r in range(requests):
        ranks.append(rank)
        rank = rank + present[r : r + 1]
    rank = jnp.concatenate(ranks, axis=0)
    slot = (column % SLOTS).astype(f32)
    mine = jnp.where(rank == slot, present, 0.0)
    return mine, mine * live0, mine * live1


def box_kernel(queries, shelf_ids, live_mask, box):
    requests, width = queries.shape
    owners = box.shape[0]
    mine, live0, live1 = choose(shelf_ids[...], live_mask[...], owners)
    dead0 = live1 * (1.0 - live0)
    dead1 = live0 * (1.0 - live1)
    lane = lax.broadcasted_iota(jnp.int32, (requests, LANES), 1)
    rows = dot(mine.astype(bf16), queries[...], ((0,), (0,)))
    flags = dot(
        jnp.concatenate([dead0, dead1], axis=0).astype(bf16),
        jnp.concatenate([(lane == 0).astype(f32), (lane == 1).astype(f32)], axis=0).astype(bf16),
        ((0,), (0,)),
    )
    both = jnp.concatenate([rows, flags], axis=1).astype(bf16)
    box[...] = both.reshape(box.shape)


def shelf_kernel(box, keys, values, out):
    senders, slots, wide = box.shape
    rows = senders * slots
    width = wide - LANES
    passages, length, _ = keys.shape
    positions = passages * length
    got = box[...].reshape(rows, wide)
    flags = got[:, width:]
    key_rows = keys[...].reshape(positions, width)
    value_rows = values[...].reshape(positions, width)
    place = lax.broadcasted_iota(jnp.int32, (positions, LANES), 0) // length
    lane = lax.broadcasted_iota(jnp.int32, (positions, LANES), 1)
    bias = jnp.where(place == lane, far_below, 0.0).astype(bf16)
    ones = jnp.ones((positions, LANES), bf16)
    stat_lane = lax.broadcasted_iota(jnp.int32, (rows, LANES), 1)
    low = stat_lane < DK
    keep = [jnp.where(low, 1.0, 0.0).astype(bf16), jnp.where(low, 0.0, 1.0).astype(bf16)]
    heads = width // DK
    stats = jnp.zeros((rows, LANES), f32)
    contexts = []
    for pair in range(width // LANES):
        at = pair * LANES
        query_pair = got[:, at : at + LANES]
        key_pair = jnp.concatenate([key_rows[:, at : at + LANES], bias], axis=1)
        value_pair = jnp.concatenate([value_rows[:, at : at + LANES], ones], axis=1)
        halves = []
        for half in range(2):
            query = query_pair * keep[half]
            scores = dot(jnp.concatenate([query, flags], axis=1), key_pair, ((1,), (1,)))
            peak = jnp.max(scores, axis=1, keepdims=True).astype(bf16).astype(f32)
            weights = jnp.exp(scores - peak).astype(bf16)
            summed = dot(weights, value_pair, ((1,), (0,)))
            total = summed[:, LANES:]
            halves.append(summed[:, :LANES] / total)
            high = total.astype(bf16).astype(f32)
            head = 2 * pair + half
            stats = jnp.where(stat_lane == head, peak, stats)
            stats = jnp.where(stat_lane == heads + head, high, stats)
            stats = jnp.where(stat_lane == 2 * heads + head, total - high, stats)
        contexts.append(jnp.where(low, halves[0], halves[1]).astype(bf16))
    both = jnp.concatenate(contexts + [stats.astype(bf16)], axis=1)
    out[...] = both.reshape(out.shape)


def merge_kernel(box, shelf_ids, live_mask, w_out, out):
    owners, slots, wide = box.shape
    rows = owners * slots
    width = wide - LANES
    heads = width // DK
    requests = shelf_ids.shape[0]
    mine, live0, live1 = choose(shelf_ids[...], live_mask[...], owners)
    read = (live0 + live1) > 0.0
    got = box[...].reshape(rows, wide)
    stats = got[:, width:].astype(f32).T
    shares = []
    totals = []
    for h in range(heads):
        peak = jnp.where(read, stats[h : h + 1], far_below)
        best = jnp.max(peak, axis=1, keepdims=True)
        total = stats[heads + h : heads + h + 1] + stats[2 * heads + h : 2 * heads + h + 1]
        share = jnp.where(read, total * jnp.exp(peak - best), 0.0)
        shares.append(share)
        totals.append(jnp.sum(share, axis=1, keepdims=True))
    share = jnp.concatenate(shares, axis=0)
    high = share.astype(bf16)
    rest = (share - high.astype(f32)).astype(bf16)
    context = got[:, :width]
    summed = dot(high, context, ((1,), (0,))) + dot(rest, context, ((1,), (0,)))
    head_of = lax.broadcasted_iota(jnp.int32, (requests, width), 1) // DK
    attended = jnp.zeros((requests, width), f32)
    for h in range(heads):
        part = summed[h * requests : (h + 1) * requests] / totals[h]
        attended = jnp.where(head_of == h, part, attended)
    attended = attended.astype(bf16)
    groups, _, columns = out.shape
    for g in range(groups):
        out[g] = dot(attended, w_out[:, g * columns : (g + 1) * columns], ((1,), (0,)))


def vmem(n):
    return [pl.BlockSpec(memory_space=pltpu.VMEM)] * n


def per_device(queries, passage_keys, passage_values, shelf_ids, live_mask, w_out):
    owners = lax.axis_size("psg")
    groups = lax.axis_size("head")
    requests, width = queries.shape
    wide = width + LANES
    box_shape = jax.ShapeDtypeStruct((owners, SLOTS, wide), bf16)
    out_spec = pl.BlockSpec(memory_space=pltpu.VMEM)

    def exchanged(x):
        return lax.all_to_all(
            x, "psg", split_axis=0, concat_axis=0, axis_index_groups=rotated_group(owners), tiled=True
        )

    box = pl.pallas_call(
        box_kernel, out_shape=box_shape, in_specs=vmem(3), out_specs=out_spec, name="box"
    )(queries, shelf_ids, live_mask)
    partials = pl.pallas_call(
        shelf_kernel, out_shape=box_shape, in_specs=vmem(3), out_specs=out_spec, name="shelf"
    )(exchanged(box), passage_keys, passage_values)
    projected = pl.pallas_call(
        merge_kernel,
        out_shape=jax.ShapeDtypeStruct((groups, requests, w_out.shape[1] // groups), f32),
        in_specs=vmem(4),
        out_specs=out_spec,
        name="merge",
    )(exchanged(partials), shelf_ids, live_mask, w_out)
    blocks = lax.all_to_all(projected, "head", 0, 0, tiled=True)
    return jnp.sum(blocks, axis=0).astype(bf16)


def solution(mesh):
    in_specs = (
        P("psg", "head"),
        P("psg", None, "head"),
        P("psg", None, "head"),
        P("psg", None),
        P("psg", None),
        P("head", None),
    )
    out_specs = P("psg", "head")
    return jax.shard_map(
        per_device, mesh=mesh, in_specs=in_specs, out_specs=out_specs, check_vma=False
    )
```

```python
import jax
import jax.numpy as jnp
from jax import lax
from jax.experimental import pallas as pl
from jax.experimental.pallas import tpu as pltpu
from jax.sharding import PartitionSpec as P

DK = 64
SLOTS = 2
LANES = 128
KERNEL_VMEM = 24 << 20
far_below = -1e30
bf16 = jnp.bfloat16
f32 = jnp.float32


def first_member(owners):
    return owners // 2 + owners // 32 + 1 if owners >= 32 else 0


def rotated_group(owners):
    first = first_member(owners)
    return [[(first + i) % owners for i in range(owners)]]


def dot(a, b, dims):
    return lax.dot_general(a, b, (dims, ((), ())), preferred_element_type=f32)


def choose(shelf_ids, live_mask, owners):
    requests, shelves = shelf_ids.shape
    columns = owners * SLOTS
    column = lax.broadcasted_iota(jnp.int32, (requests, columns), 1)
    position = column // SLOTS + first_member(owners)
    owner = jnp.where(position >= owners, position - owners, position)
    present = jnp.zeros((requests, columns), f32)
    live0 = jnp.zeros((requests, columns), f32)
    live1 = jnp.zeros((requests, columns), f32)
    for j in range(shelves):
        hit = (shelf_ids[:, j : j + 1] == owner).astype(f32)
        present = present + hit
        first = live_mask[:, 2 * j : 2 * j + 1].astype(f32)
        first = jnp.ones_like(first) if j == 0 else first
        live0 = live0 + hit * first
        live1 = live1 + hit * live_mask[:, 2 * j + 1 : 2 * j + 2].astype(f32)
    rank = jnp.zeros((1, columns), f32)
    ranks = []
    for r in range(requests):
        ranks.append(rank)
        rank = rank + present[r : r + 1]
    rank = jnp.concatenate(ranks, axis=0)
    slot = (column % SLOTS).astype(f32)
    mine = jnp.where(rank == slot, present, 0.0)
    return mine, mine * live0, mine * live1


def box_kernel(queries, shelf_ids, live_mask, box):
    requests, width = queries.shape
    owners = box.shape[0]
    mine, live0, live1 = choose(shelf_ids[...], live_mask[...], owners)
    dead0 = live1 * (1.0 - live0)
    dead1 = live0 * (1.0 - live1)
    lane = lax.broadcasted_iota(jnp.int32, (requests, LANES), 1)
    rows = dot(mine.astype(bf16), queries[...], ((0,), (0,)))
    flags = dot(
        jnp.concatenate([dead0, dead1], axis=0).astype(bf16),
        jnp.concatenate([(lane == 0).astype(f32), (lane == 1).astype(f32)], axis=0).astype(bf16),
        ((0,), (0,)),
    )
    both = jnp.concatenate([rows, flags], axis=1).astype(bf16)
    box[...] = both.reshape(box.shape)


def shelf_kernel(box, keys, values, out):
    senders, slots, wide = box.shape
    rows = senders * slots
    width = wide - LANES
    passages, length, _ = keys.shape
    positions = passages * length
    got = box[...].reshape(rows, wide)
    flags = got[:, width:]
    key_rows = keys[...].reshape(positions, width)
    value_rows = values[...].reshape(positions, width)
    place = lax.broadcasted_iota(jnp.int32, (positions, LANES), 0) // length
    lane = lax.broadcasted_iota(jnp.int32, (positions, LANES), 1)
    bias = jnp.where(place == lane, far_below, 0.0).astype(bf16)
    ones = jnp.ones((positions, LANES), bf16)
    stat_lane = lax.broadcasted_iota(jnp.int32, (rows, LANES), 1)
    low = stat_lane < DK
    keep = [jnp.where(low, 1.0, 0.0).astype(bf16), jnp.where(low, 0.0, 1.0).astype(bf16)]
    heads = width // DK
    stats = jnp.zeros((rows, LANES), f32)
    contexts = []
    for pair in range(width // LANES):
        at = pair * LANES
        query_pair = got[:, at : at + LANES]
        key_pair = jnp.concatenate([key_rows[:, at : at + LANES], bias], axis=1)
        value_pair = jnp.concatenate([value_rows[:, at : at + LANES], ones], axis=1)
        halves = []
        for half in range(2):
            query = query_pair * keep[half]
            scores = dot(jnp.concatenate([query, flags], axis=1), key_pair, ((1,), (1,)))
            peak = jnp.max(scores, axis=1, keepdims=True).astype(bf16).astype(f32)
            weights = jnp.exp(scores - peak).astype(bf16)
            summed = dot(weights, value_pair, ((1,), (0,)))
            total = summed[:, LANES:]
            halves.append(summed[:, :LANES] / total)
            high = total.astype(bf16).astype(f32)
            head = 2 * pair + half
            stats = jnp.where(stat_lane == head, peak, stats)
            stats = jnp.where(stat_lane == heads + head, high, stats)
            stats = jnp.where(stat_lane == 2 * heads + head, total - high, stats)
        contexts.append(jnp.where(low, halves[0], halves[1]).astype(bf16))
    both = jnp.concatenate(contexts + [stats.astype(bf16)], axis=1)
    out[...] = both.reshape(out.shape)


def merge_kernel(box, shelf_ids, live_mask, w_out, out):
    owners, slots, wide = box.shape
    rows = owners * slots
    width = wide - LANES
    heads = width // DK
    requests = shelf_ids.shape[0]
    mine, live0, live1 = choose(shelf_ids[...], live_mask[...], owners)
    read = (live0 + live1) > 0.0
    got = box[...].reshape(rows, wide)
    stats = got[:, width:].astype(f32).T
    shares = []
    totals = []
    for h in range(heads):
        peak = jnp.where(read, stats[h : h + 1], far_below)
        best = jnp.max(peak, axis=1, keepdims=True)
        total = stats[heads + h : heads + h + 1] + stats[2 * heads + h : 2 * heads + h + 1]
        share = jnp.where(read, total * jnp.exp(peak - best), 0.0)
        shares.append(share)
        totals.append(jnp.sum(share, axis=1, keepdims=True))
    share = jnp.concatenate(shares, axis=0)
    high = share.astype(bf16)
    rest = (share - high.astype(f32)).astype(bf16)
    context = got[:, :width]
    summed = dot(high, context, ((1,), (0,))) + dot(rest, context, ((1,), (0,)))
    head_of = lax.broadcasted_iota(jnp.int32, (requests, width), 1) // DK
    attended = jnp.zeros((requests, width), f32)
    for h in range(heads):
        part = summed[h * requests : (h + 1) * requests] / totals[h]
        attended = jnp.where(head_of == h, part, attended)
    attended = attended.astype(bf16)
    groups, _, columns = out.shape
    for g in range(groups):
        out[g] = dot(attended, w_out[:, g * columns : (g + 1) * columns], ((1,), (0,)))


def stage_kernel(*refs):
    count = (len(refs) - 1) // 2
    copies = [
        pltpu.make_async_copy(refs[n], refs[count + n], refs[-1].at[n]) for n in range(count)
    ]
    for copy in copies:
        copy.start()
    for copy in copies:
        copy.wait()


def in_vmem(shape, dtype):
    return pltpu.VMEM(shape, dtype)


def staged(*arrays):
    return pl.pallas_call(
        stage_kernel,
        out_shape=[in_vmem(a.shape, a.dtype) for a in arrays],
        in_specs=[pl.BlockSpec(memory_space=pl.ANY)] * len(arrays),
        out_specs=[pl.BlockSpec(memory_space=pltpu.VMEM)] * len(arrays),
        scratch_shapes=[pltpu.SemaphoreType.DMA((len(arrays),))],
        compiler_params=pltpu.CompilerParams(vmem_limit_bytes=1 << 20),
        name="stage",
    )(*[pltpu.with_memory_space_constraint(a, pltpu.HBM) for a in arrays])


def call(kernel, shape, dtype, name, near, far=()):
    spec = pl.BlockSpec(memory_space=pltpu.VMEM)
    near = [pltpu.with_memory_space_constraint(a, pltpu.VMEM) for a in near]
    far = [pltpu.with_memory_space_constraint(a, pltpu.HBM) for a in far]
    return pl.pallas_call(
        kernel,
        out_shape=in_vmem(shape, dtype),
        in_specs=[spec] * (len(near) + len(far)),
        out_specs=spec,
        compiler_params=pltpu.CompilerParams(vmem_limit_bytes=KERNEL_VMEM),
        name=name,
    )(*near, *far)


def per_device(queries, passage_keys, passage_values, shelf_ids, live_mask, w_out):
    owners = lax.axis_size("psg")
    groups = lax.axis_size("head")
    requests, width = queries.shape
    wide = width + LANES
    def exchanged(x):
        return lax.all_to_all(
            x, "psg", split_axis=0, concat_axis=0, axis_index_groups=rotated_group(owners), tiled=True
        )

    box_shape = (owners, SLOTS, wide)
    box = call(box_kernel, box_shape, bf16, "box", (), (queries, shelf_ids, live_mask))
    keys, values, w_near, ids_near, live_near = staged(
        passage_keys, passage_values, w_out, shelf_ids, live_mask
    )
    partials = call(shelf_kernel, box_shape, bf16, "shelf", (exchanged(box), keys, values))
    projected = call(
        merge_kernel,
        (groups, requests, w_out.shape[1] // groups),
        f32,
        "merge",
        (exchanged(partials), ids_near, live_near, w_near),
    )
    blocks = lax.all_to_all(projected, "head", 0, 0, tiled=True)
    return jnp.sum(blocks, axis=0).astype(bf16)


def solution(mesh):
    in_specs = (
        P("psg", "head"),
        P("psg", None, "head"),
        P("psg", None, "head"),
        P("psg", None),
        P("psg", None),
        P("head", None),
    )
    out_specs = P("psg", "head")
    return jax.shard_map(
        per_device, mesh=mesh, in_specs=in_specs, out_specs=out_specs, check_vma=False
    )
```

```python
import jax
import jax.numpy as jnp
from jax import lax
from jax.experimental import pallas as pl
from jax.experimental.pallas import tpu as pltpu
from jax.sharding import PartitionSpec as P

DK = 64
SLOTS = 2
CORES = 2
LANES = 128
KERNEL_VMEM = 24 << 20
far_below = -1e30
bf16 = jnp.bfloat16
f32 = jnp.float32


def first_chip(chips):
    return chips // 2 + chips // 32 if chips >= 32 else 0


def rotated(length, first):
    return [(first + i) % length for i in range(length)]


def same_core_groups(owners):
    chips = owners // CORES
    order = rotated(chips, first_chip(chips))
    return [[CORES * chip + core for chip in order] for core in range(CORES)]


def dot(a, b, dims):
    return lax.dot_general(a, b, (dims, ((), ())), preferred_element_type=f32)


def own_core():
    return lax.axis_index("psg") % CORES


def choose(shelf_ids, live_mask, chips, core):
    requests, shelves = shelf_ids.shape
    half = chips * SLOTS
    columns = CORES * half
    column = lax.broadcasted_iota(jnp.int32, (requests, columns), 1)
    other = (column >= half).astype(jnp.int32)
    place = (column - other * half) // SLOTS + first_chip(chips)
    chip = jnp.where(place >= chips, place - chips, place)
    owner = CORES * chip + jnp.where(other == core, 0, 1)
    present = jnp.zeros((requests, columns), f32)
    live0 = jnp.zeros((requests, columns), f32)
    live1 = jnp.zeros((requests, columns), f32)
    for j in range(shelves):
        hit = (shelf_ids[:, j : j + 1] == owner).astype(f32)
        present = present + hit
        first = live_mask[:, 2 * j : 2 * j + 1].astype(f32)
        first = jnp.ones_like(first) if j == 0 else first
        live0 = live0 + hit * first
        live1 = live1 + hit * live_mask[:, 2 * j + 1 : 2 * j + 2].astype(f32)
    rank = jnp.zeros((1, columns), f32)
    ranks = []
    for r in range(requests):
        ranks.append(rank)
        rank = rank + present[r : r + 1]
    rank = jnp.concatenate(ranks, axis=0)
    slot = (column % SLOTS).astype(f32)
    mine = jnp.where(rank == slot, present, 0.0)
    return mine, mine * live0, mine * live1


def box_kernel(queries, shelf_ids, live_mask, box):
    requests, width = queries.shape
    chips = box.shape[0]
    half = chips * SLOTS
    mine, live0, live1 = choose(shelf_ids[...], live_mask[...], chips, own_core())
    dead0 = live1 * (1.0 - live0)
    dead1 = live0 * (1.0 - live1)
    dead = [dead0[:, :half], dead1[:, :half], dead0[:, half:], dead1[:, half:]]
    lane = lax.broadcasted_iota(jnp.int32, (requests, LANES), 1)
    rows = dot(mine.astype(bf16), queries[...], ((0,), (0,)))
    flags = dot(
        jnp.concatenate(dead, axis=0).astype(bf16),
        jnp.concatenate([(lane == n).astype(f32) for n in range(len(dead))], axis=0).astype(bf16),
        ((0,), (0,)),
    )
    both = jnp.concatenate([rows[:half], rows[half:], flags], axis=1).astype(bf16)
    box[...] = both.reshape(box.shape)


def shelf_kernel(box, keys, values, other_keys, other_values, out):
    chips, slots, wide = box.shape
    rows = chips * slots
    width = (wide - LANES) // CORES
    passages, length, _ = keys.shape
    positions = passages * length
    heads = width // DK
    got = box[...].reshape(rows, wide)
    flags = got[:, CORES * width :]
    flags = jnp.concatenate([flags, flags], axis=0)
    place = lax.broadcasted_iota(jnp.int32, (positions, LANES), 0) // length
    lane = lax.broadcasted_iota(jnp.int32, (positions, LANES), 1)
    ones = jnp.ones((positions, LANES), bf16)
    stat_lane = lax.broadcasted_iota(jnp.int32, (rows, LANES), 1)
    low = stat_lane < DK
    keep = [jnp.where(low, 1.0, 0.0).astype(bf16), jnp.where(low, 0.0, 1.0).astype(bf16)]
    stats = jnp.zeros((rows, LANES), f32)
    contexts = []
    for shelf, (key_ref, value_ref) in enumerate(((keys, values), (other_keys, other_values))):
        bias = jnp.where(place + passages * shelf == lane, far_below, 0.0).astype(bf16)
        key_rows = key_ref[...].reshape(positions, width)
        value_rows = value_ref[...].reshape(positions, width)
        for pair in range(width // LANES):
            at = pair * LANES
            query_pair = got[:, shelf * width + at : shelf * width + at + LANES]
            query = jnp.concatenate([query_pair * keep[0], query_pair * keep[1]], axis=0)
            key_pair = jnp.concatenate([key_rows[:, at : at + LANES], bias], axis=1)
            value_pair = jnp.concatenate([value_rows[:, at : at + LANES], ones], axis=1)
            scores = dot(jnp.concatenate([query, flags], axis=1), key_pair, ((1,), (1,)))
            peak = jnp.max(scores, axis=1, keepdims=True).astype(bf16).astype(f32)
            weights = jnp.exp(scores - peak).astype(bf16)
            summed = dot(weights, value_pair, ((1,), (0,)))
            total = summed[:, LANES:]
            context = summed[:, :LANES] / total
            contexts.append(jnp.where(low, context[:rows], context[rows:]).astype(bf16))
            high = total.astype(bf16).astype(f32)
            for part in range(2):
                own = slice(part * rows, (part + 1) * rows)
                at_lane = 3 * heads * shelf + 2 * pair + part
                stats = jnp.where(stat_lane == at_lane, peak[own], stats)
                stats = jnp.where(stat_lane == at_lane + heads, high[own], stats)
                stats = jnp.where(stat_lane == at_lane + 2 * heads, (total - high)[own], stats)
    both = jnp.concatenate(contexts + [stats.astype(bf16)], axis=1)
    out[...] = both.reshape(out.shape)


def merge_kernel(box, shelf_ids, live_mask, w_first, w_out, out, w_rest, arrived):
    rest_copy = pltpu.make_async_copy(w_out.at[:, w_first.shape[1] :], w_rest, arrived)
    rest_copy.start()
    chips, slots, wide = box.shape
    rows = chips * slots
    width = (wide - LANES) // CORES
    heads = width // DK
    requests = shelf_ids.shape[0]
    mine, live0, live1 = choose(shelf_ids[...], live_mask[...], chips, own_core())
    read = (live0 + live1) > 0.0
    got = box[...].reshape(rows, wide)
    stats = got[:, CORES * width :].astype(f32).T

    def stat(n):
        return jnp.concatenate([stats[n : n + 1], stats[3 * heads + n : 3 * heads + n + 1]], axis=1)

    shares = []
    totals = []
    for h in range(heads):
        peak = jnp.where(read, stat(h), far_below)
        best = jnp.max(peak, axis=1, keepdims=True)
        total = stat(heads + h) + stat(2 * heads + h)
        share = jnp.where(read, total * jnp.exp(peak - best), 0.0)
        shares.append(share)
        totals.append(jnp.sum(share, axis=1, keepdims=True))
    share = jnp.concatenate(shares, axis=0)
    high = share.astype(bf16)
    rest = (share - high.astype(f32)).astype(bf16)
    context = jnp.concatenate([got[:, :width], got[:, width : 2 * width]], axis=0)
    summed = dot(high, context, ((1,), (0,))) + dot(rest, context, ((1,), (0,)))
    head_of = lax.broadcasted_iota(jnp.int32, (requests, width), 1) // DK
    attended = jnp.zeros((requests, width), f32)
    for h in range(heads):
        part = summed[h * requests : (h + 1) * requests] / totals[h]
        attended = jnp.where(head_of == h, part, attended)
    attended = attended.astype(bf16)
    groups, _, columns = out.shape
    ahead = w_first.shape[1] // columns
    order = rotated(groups, groups // 2)
    for g in range(groups):
        if g == ahead:
            rest_copy.wait()
        at = g * columns if g < ahead else (g - ahead) * columns
        weights = (w_first if g < ahead else w_rest)[:, at : at + columns]
        out[order.index(g)] = dot(attended, weights, ((1,), (0,)))


def stage_kernel(*refs):
    count = (len(refs) - 1) // 2
    copies = [
        pltpu.make_async_copy(
            refs[n].at[tuple(pl.ds(0, k) for k in refs[count + n].shape)],
            refs[count + n],
            refs[-1].at[n],
        )
        for n in range(count)
    ]
    for copy in copies:
        copy.start()
    for copy in copies:
        copy.wait()


def in_vmem(shape, dtype):
    return pltpu.VMEM(shape, dtype)


def staged(shapes, arrays):
    return pl.pallas_call(
        stage_kernel,
        out_shape=[in_vmem(shape, a.dtype) for shape, a in zip(shapes, arrays)],
        in_specs=[pl.BlockSpec(memory_space=pl.ANY)] * len(arrays),
        out_specs=[pl.BlockSpec(memory_space=pltpu.VMEM)] * len(arrays),
        scratch_shapes=[pltpu.SemaphoreType.DMA((len(arrays),))],
        compiler_params=pltpu.CompilerParams(vmem_limit_bytes=1 << 20),
        name="stage",
    )(*[pltpu.with_memory_space_constraint(a, pltpu.HBM) for a in arrays])


def call(kernel, shape, dtype, name, near, far=(), hbm=(), scratch=()):
    spec = pl.BlockSpec(memory_space=pltpu.VMEM)
    near = [pltpu.with_memory_space_constraint(a, pltpu.VMEM) for a in near]
    far, hbm = [[pltpu.with_memory_space_constraint(a, pltpu.HBM) for a in some] for some in (far, hbm)]
    return pl.pallas_call(
        kernel,
        out_shape=in_vmem(shape, dtype),
        in_specs=[spec] * (len(near) + len(far)) + [pl.BlockSpec(memory_space=pl.ANY)] * len(hbm),
        out_specs=spec,
        scratch_shapes=list(scratch),
        compiler_params=pltpu.CompilerParams(vmem_limit_bytes=KERNEL_VMEM),
        name=name,
    )(*near, *far, *hbm)


def per_device(queries, passage_keys, passage_values, shelf_ids, live_mask, w_out):
    owners = lax.axis_size("psg")
    groups = lax.axis_size("head")
    requests, width = queries.shape

    def exchanged(x, axis, index_groups):
        return lax.all_to_all(
            x, axis, split_axis=0, concat_axis=0, axis_index_groups=index_groups, tiled=True
        )

    def from_other_core(x):
        return lax.ppermute(x, "psg", [(i, i ^ 1) for i in range(owners)])

    same_core = same_core_groups(owners)
    box_shape = (owners // CORES, SLOTS, CORES * width + LANES)
    box = call(box_kernel, box_shape, bf16, "box", (), (queries, shelf_ids, live_mask))
    ready = (passage_keys, passage_values, shelf_ids, live_mask, w_out)
    depth, columns = w_out.shape
    shapes = [a.shape for a in ready[:-1]] + [(depth, columns // 2)]
    keys, values, ids_near, live_near, w_first = staged(shapes, ready)
    partials = call(
        shelf_kernel,
        box_shape,
        bf16,
        "shelf",
        (
            exchanged(box, "psg", same_core),
            keys,
            values,
            from_other_core(passage_keys),
            from_other_core(passage_values),
        ),
    )
    projected = call(
        merge_kernel,
        (groups, requests, columns // groups),
        f32,
        "merge",
        (exchanged(partials, "psg", same_core), ids_near, live_near, w_first),
        hbm=(w_out,),
        scratch=(pltpu.VMEM((depth, columns - columns // 2), bf16), pltpu.SemaphoreType.DMA),
    )
    blocks = exchanged(projected, "head", [rotated(groups, groups // 2)])
    return jnp.sum(blocks, axis=0).astype(bf16)


def solution(mesh):
    in_specs = (
        P("psg", "head"),
        P("psg", None, "head"),
        P("psg", None, "head"),
        P("psg", None),
        P("psg", None),
        P("head", None),
    )
    out_specs = P("psg", "head")
    return jax.shard_map(
        per_device, mesh=mesh, in_specs=in_specs, out_specs=out_specs, check_vma=False
    )
```

```python
import jax
import jax.numpy as jnp
from jax import lax
from jax.experimental import pallas as pl
from jax.experimental.pallas import tpu as pltpu
from jax.sharding import PartitionSpec as P

DK = 64
SLOTS = 2
CORES = 2
LANES = 128
KERNEL_VMEM = 24 << 20
far_below = -1e30
bf16 = jnp.bfloat16
f32 = jnp.float32


def first_chip(chips):
    return chips * 45 // 64 if chips >= 32 else 0


def rotated(length, first):
    return [(first + i) % length for i in range(length)]


def same_core_groups(owners):
    chips = owners // CORES
    order = rotated(chips, first_chip(chips))
    return [[CORES * chip + core for chip in order] for core in range(CORES)]


def dot(a, b, dims):
    return lax.dot_general(a, b, (dims, ((), ())), preferred_element_type=f32)


def own_core():
    return lax.axis_index("psg") % CORES


def choose(shelf_ids, live_mask, chips, core):
    requests, shelves = shelf_ids.shape
    half = chips * SLOTS
    columns = CORES * half
    column = lax.broadcasted_iota(jnp.int32, (requests, columns), 1)
    other = (column >= half).astype(jnp.int32)
    place = (column - other * half) // SLOTS + first_chip(chips)
    chip = jnp.where(place >= chips, place - chips, place)
    owner = CORES * chip + jnp.where(other == core, 0, 1)
    present = jnp.zeros((requests, columns), f32)
    live0 = jnp.zeros((requests, columns), f32)
    live1 = jnp.zeros((requests, columns), f32)
    for j in range(shelves):
        hit = (shelf_ids[:, j : j + 1] == owner).astype(f32)
        present = present + hit
        first = live_mask[:, 2 * j : 2 * j + 1].astype(f32)
        first = jnp.ones_like(first) if j == 0 else first
        live0 = live0 + hit * first
        live1 = live1 + hit * live_mask[:, 2 * j + 1 : 2 * j + 2].astype(f32)
    rank = jnp.zeros((1, columns), f32)
    ranks = []
    for r in range(requests):
        ranks.append(rank)
        rank = rank + present[r : r + 1]
    rank = jnp.concatenate(ranks, axis=0)
    slot = (column % SLOTS).astype(f32)
    mine = jnp.where(rank == slot, present, 0.0)
    return mine, mine * live0, mine * live1


def box_kernel(queries, shelf_ids, live_mask, box):
    requests, width = queries.shape
    chips = box.shape[0]
    half = chips * SLOTS
    mine, live0, live1 = choose(shelf_ids[...], live_mask[...], chips, own_core())
    dead0 = live1 * (1.0 - live0)
    dead1 = live0 * (1.0 - live1)
    dead = [dead0[:, :half], dead1[:, :half], dead0[:, half:], dead1[:, half:]]
    lane = lax.broadcasted_iota(jnp.int32, (requests, LANES), 1)
    rows = dot(mine.astype(bf16), queries[...], ((0,), (0,)))
    flags = dot(
        jnp.concatenate(dead, axis=0).astype(bf16),
        jnp.concatenate([(lane == n).astype(f32) for n in range(len(dead))], axis=0).astype(bf16),
        ((0,), (0,)),
    )
    both = jnp.concatenate([rows[:half], rows[half:], flags], axis=1).astype(bf16)
    box[...] = both.reshape(box.shape)


def shelf_kernel(box, keys, values, other_keys, other_values, w_out, out, w_near, got, arrived):
    w_copy = pltpu.make_async_copy(w_out, w_near, arrived)
    w_copy.start()
    chips, slots, wide = box.shape
    rows = chips * slots
    width = (wide - LANES) // CORES
    passages, length, _ = keys.shape
    positions = passages * length
    heads = width // DK
    got[...] = box[...].reshape(rows, wide)
    flags = got[:, CORES * width :]
    flags = jnp.concatenate([flags, flags], axis=0)
    place = lax.broadcasted_iota(jnp.int32, (positions, LANES), 0) // length
    lane = lax.broadcasted_iota(jnp.int32, (positions, LANES), 1)
    ones = jnp.ones((positions, LANES), bf16)
    stat_lane = lax.broadcasted_iota(jnp.int32, (rows, LANES), 1)
    low = stat_lane < DK
    keep = [jnp.where(low, 1.0, 0.0).astype(bf16), jnp.where(low, 0.0, 1.0).astype(bf16)]
    stats = jnp.zeros((rows, LANES), f32)
    contexts = []
    for shelf, (key_ref, value_ref) in enumerate(((keys, values), (other_keys, other_values))):
        bias = jnp.where(place + passages * shelf == lane, far_below, 0.0).astype(bf16)
        key_rows = key_ref[...].reshape(positions, width)
        value_rows = value_ref[...].reshape(positions, width)
        for pair in range(width // LANES):
            at = pair * LANES
            query_pair = got[:, shelf * width + at : shelf * width + at + LANES]
            query = jnp.concatenate([query_pair * keep[0], query_pair * keep[1]], axis=0)
            key_pair = jnp.concatenate([key_rows[:, at : at + LANES], bias], axis=1)
            value_pair = jnp.concatenate([value_rows[:, at : at + LANES], ones], axis=1)
            scores = dot(jnp.concatenate([query, flags], axis=1), key_pair, ((1,), (1,)))
            peak = jnp.max(scores, axis=1, keepdims=True).astype(bf16).astype(f32)
            weights = jnp.exp(scores - peak).astype(bf16)
            summed = dot(weights, value_pair, ((1,), (0,)))
            total = summed[:, LANES:]
            context = summed[:, :LANES] / total
            contexts.append(jnp.where(low, context[:rows], context[rows:]).astype(bf16))
            high = total.astype(bf16).astype(f32)
            for part in range(2):
                own = slice(part * rows, (part + 1) * rows)
                at_lane = 3 * heads * shelf + 2 * pair + part
                stats = jnp.where(stat_lane == at_lane, peak[own], stats)
                stats = jnp.where(stat_lane == at_lane + heads, high[own], stats)
                stats = jnp.where(stat_lane == at_lane + 2 * heads, (total - high)[own], stats)
    both = jnp.concatenate(contexts + [stats.astype(bf16)], axis=1)
    out[...] = both.reshape(out.shape)
    w_copy.wait()


def merge_kernel(box, w_out, shelf_ids, live_mask, out, got):
    chips, slots, wide = box.shape
    rows = chips * slots
    width = (wide - LANES) // CORES
    heads = width // DK
    requests = shelf_ids.shape[0]
    mine, live0, live1 = choose(shelf_ids[...], live_mask[...], chips, own_core())
    read = (live0 + live1) > 0.0
    got[...] = box[...].reshape(rows, wide)
    stats = got[:, CORES * width :].astype(f32).T

    def stat(n):
        return jnp.concatenate([stats[n : n + 1], stats[3 * heads + n : 3 * heads + n + 1]], axis=1)

    shares = []
    totals = []
    for h in range(heads):
        peak = jnp.where(read, stat(h), far_below)
        best = jnp.max(peak, axis=1, keepdims=True)
        total = stat(heads + h) + stat(2 * heads + h)
        share = jnp.where(read, total * jnp.exp(peak - best), 0.0)
        shares.append(share)
        totals.append(jnp.sum(share, axis=1, keepdims=True))
    share = jnp.concatenate(shares, axis=0)
    high = share.astype(bf16)
    rest = (share - high.astype(f32)).astype(bf16)
    context = jnp.concatenate([got[:, :width], got[:, width : 2 * width]], axis=0)
    summed = dot(high, context, ((1,), (0,))) + dot(rest, context, ((1,), (0,)))
    head_of = lax.broadcasted_iota(jnp.int32, (requests, width), 1) // DK
    attended = jnp.zeros((requests, width), f32)
    for h in range(heads):
        part = summed[h * requests : (h + 1) * requests] / totals[h]
        attended = jnp.where(head_of == h, part, attended)
    attended = attended.astype(bf16)
    groups, _, columns = out.shape
    for n, g in enumerate(rotated(groups, groups // 2)):
        out[n] = dot(attended, w_out[:, g * columns : (g + 1) * columns], ((1,), (0,)))


def stage_kernel(*refs):
    count = (len(refs) - 1) // 2
    copies = [
        pltpu.make_async_copy(
            refs[n].at[tuple(pl.ds(0, k) for k in refs[count + n].shape)],
            refs[count + n],
            refs[-1].at[n],
        )
        for n in range(count)
    ]
    for copy in copies:
        copy.start()
    for copy in copies:
        copy.wait()


def in_vmem(shape, dtype):
    return pltpu.VMEM(shape, dtype)


def staged(*arrays):
    return pl.pallas_call(
        stage_kernel,
        out_shape=[in_vmem(a.shape, a.dtype) for a in arrays],
        in_specs=[pl.BlockSpec(memory_space=pl.ANY)] * len(arrays),
        out_specs=[pl.BlockSpec(memory_space=pltpu.VMEM)] * len(arrays),
        scratch_shapes=[pltpu.SemaphoreType.DMA((len(arrays),))],
        compiler_params=pltpu.CompilerParams(vmem_limit_bytes=1 << 20),
        name="stage",
    )(*[pltpu.with_memory_space_constraint(a, pltpu.HBM) for a in arrays])


def call(kernel, results, name, near, far=(), hbm=(), scratch=()):
    spec = pl.BlockSpec(memory_space=pltpu.VMEM)
    near = [pltpu.with_memory_space_constraint(a, pltpu.VMEM) for a in near]
    far, hbm = [
        [pltpu.with_memory_space_constraint(a, pltpu.HBM) for a in some] for some in (far, hbm)
    ]
    return pl.pallas_call(
        kernel,
        out_shape=[in_vmem(*result) for result in results],
        in_specs=[spec] * (len(near) + len(far)) + [pl.BlockSpec(memory_space=pl.ANY)] * len(hbm),
        out_specs=[spec] * len(results),
        scratch_shapes=list(scratch),
        compiler_params=pltpu.CompilerParams(vmem_limit_bytes=KERNEL_VMEM),
        name=name,
    )(*near, *far, *hbm)


def per_device(queries, passage_keys, passage_values, shelf_ids, live_mask, w_out):
    owners = lax.axis_size("psg")
    groups = lax.axis_size("head")
    requests, width = queries.shape

    def exchanged(x, axis, index_groups):
        return lax.all_to_all(
            x, axis, split_axis=0, concat_axis=0, axis_index_groups=index_groups, tiled=True
        )

    def from_other_core(x):
        return lax.ppermute(x, "psg", [(i, i ^ 1) for i in range(owners)])

    same_core = same_core_groups(owners)
    chips = owners // CORES
    wide = CORES * width + LANES
    box_array = ((chips, SLOTS, wide), bf16)
    rows = pltpu.VMEM((chips * SLOTS, wide), bf16)
    (box,) = call(box_kernel, [box_array], "box", (), (queries, shelf_ids, live_mask))
    keys, values, ids_near, live_near = staged(passage_keys, passage_values, shelf_ids, live_mask)
    partials, w_near = call(
        shelf_kernel,
        [box_array, (w_out.shape, w_out.dtype)],
        "shelf",
        (
            exchanged(box, "psg", same_core),
            keys,
            values,
            from_other_core(passage_keys),
            from_other_core(passage_values),
        ),
        hbm=(w_out,),
        scratch=(rows, pltpu.SemaphoreType.DMA),
    )
    (projected,) = call(
        merge_kernel,
        [((groups, requests, w_out.shape[1] // groups), f32)],
        "merge",
        (exchanged(partials, "psg", same_core), w_near, ids_near, live_near),
        scratch=(rows,),
    )
    blocks = exchanged(projected, "head", [rotated(groups, groups // 2)])
    return jnp.sum(blocks, axis=0).astype(bf16)


def solution(mesh):
    in_specs = (
        P("psg", "head"),
        P("psg", None, "head"),
        P("psg", None, "head"),
        P("psg", None),
        P("psg", None),
        P("head", None),
    )
    out_specs = P("psg", "head")
    return jax.shard_map(
        per_device, mesh=mesh, in_specs=in_specs, out_specs=out_specs, check_vma=False
    )
```

```python
import jax
import jax.numpy as jnp
from jax import lax
from jax.experimental import pallas as pl
from jax.experimental.pallas import tpu as pltpu
from jax.sharding import PartitionSpec as P

DK = 64
SLOTS = 2
CORES = 2
LANES = 128
KERNEL_VMEM = 24 << 20
far_below = -1e30
bf16 = jnp.bfloat16
f32 = jnp.float32


def first_chip(chips):
    return chips * 45 // 64 if chips >= 32 else 0


def rotated(length, first):
    return [(first + i) % length for i in range(length)]


def same_core_groups(owners):
    chips = owners // CORES
    order = rotated(chips, first_chip(chips))
    return [[CORES * chip + core for chip in order] for core in range(CORES)]


def dot(a, b, dims):
    return lax.dot_general(a, b, (dims, ((), ())), preferred_element_type=f32)


def own_core():
    return lax.axis_index("psg") % CORES


def choose(shelf_ids, live_mask, chips, core):
    requests, shelves = shelf_ids.shape
    half = chips * SLOTS
    columns = CORES * half
    column = lax.broadcasted_iota(jnp.int32, (requests, columns), 1)
    other = (column >= half).astype(jnp.int32)
    place = (column - other * half) // SLOTS + first_chip(chips)
    chip = jnp.where(place >= chips, place - chips, place)
    owner = CORES * chip + jnp.where(other == core, 0, 1)
    present = jnp.zeros((requests, columns), f32)
    live0 = jnp.zeros((requests, columns), f32)
    live1 = jnp.zeros((requests, columns), f32)
    for j in range(shelves):
        hit = (shelf_ids[:, j : j + 1] == owner).astype(f32)
        present = present + hit
        first = live_mask[:, 2 * j : 2 * j + 1].astype(f32)
        first = jnp.ones_like(first) if j == 0 else first
        live0 = live0 + hit * first
        live1 = live1 + hit * live_mask[:, 2 * j + 1 : 2 * j + 2].astype(f32)
    rank = jnp.zeros((1, columns), f32)
    ranks = []
    for r in range(requests):
        ranks.append(rank)
        rank = rank + present[r : r + 1]
    rank = jnp.concatenate(ranks, axis=0)
    slot = (column % SLOTS).astype(f32)
    mine = jnp.where(rank == slot, present, 0.0)
    return mine, mine * live0, mine * live1


def box_kernel(queries, shelf_ids, live_mask, box):
    requests, width = queries.shape
    chips = box.shape[0]
    half = chips * SLOTS
    mine, live0, live1 = choose(shelf_ids[...], live_mask[...], chips, own_core())
    dead0 = live1 * (1.0 - live0)
    dead1 = live0 * (1.0 - live1)
    dead = [dead0[:, :half], dead1[:, :half], dead0[:, half:], dead1[:, half:]]
    lane = lax.broadcasted_iota(jnp.int32, (requests, LANES), 1)
    rows = dot(mine.astype(bf16), queries[...], ((0,), (0,)))
    flags = dot(
        jnp.concatenate(dead, axis=0).astype(bf16),
        jnp.concatenate([(lane == n).astype(f32) for n in range(len(dead))], axis=0).astype(bf16),
        ((0,), (0,)),
    )
    both = jnp.concatenate([rows[:half], rows[half:], flags], axis=1).astype(bf16)
    box[...] = both.reshape(box.shape)


def shelf_kernel(box, keys, values, other_keys, other_values, w_out, out, w_near, got, arrived):
    w_copy = pltpu.make_async_copy(w_out, w_near, arrived)
    w_copy.start()
    chips, slots, wide = box.shape
    rows = chips * slots
    width = (wide - LANES) // CORES
    passages, length, _ = keys.shape
    positions = passages * length
    heads = width // DK
    got[...] = box[...].reshape(rows, wide)
    flags = got[:, CORES * width :]
    flags = jnp.concatenate([flags, flags], axis=0)
    place = lax.broadcasted_iota(jnp.int32, (positions, LANES), 0) // length
    lane = lax.broadcasted_iota(jnp.int32, (positions, LANES), 1)
    ones = jnp.ones((positions, LANES), bf16)
    stat_lane = lax.broadcasted_iota(jnp.int32, (rows, LANES), 1)
    low = stat_lane < DK
    keep = [jnp.where(low, 1.0, 0.0).astype(bf16), jnp.where(low, 0.0, 1.0).astype(bf16)]
    peaks = jnp.zeros((rows, LANES), f32)
    totals = jnp.zeros((rows, LANES), f32)
    contexts = []
    for shelf, (key_ref, value_ref) in enumerate(((keys, values), (other_keys, other_values))):
        bias = jnp.where(place + passages * shelf == lane, far_below, 0.0).astype(bf16)
        key_rows = key_ref[...].reshape(positions, width)
        value_rows = value_ref[...].reshape(positions, width)
        for pair in range(width // LANES):
            at = pair * LANES
            query_pair = got[:, shelf * width + at : shelf * width + at + LANES]
            query = jnp.concatenate([query_pair * keep[0], query_pair * keep[1]], axis=0)
            key_pair = jnp.concatenate([key_rows[:, at : at + LANES], bias], axis=1)
            value_pair = jnp.concatenate([value_rows[:, at : at + LANES], ones], axis=1)
            scores = dot(jnp.concatenate([query, flags], axis=1), key_pair, ((1,), (1,)))
            peak = jnp.max(scores, axis=1, keepdims=True).astype(bf16).astype(f32)
            weights = jnp.exp(scores - peak).astype(bf16)
            summed = dot(weights, value_pair, ((1,), (0,)))
            total = summed[:, LANES:]
            context = summed[:, :LANES] / total
            contexts.append(jnp.where(low, context[:rows], context[rows:]).astype(bf16))
            for part in range(2):
                own = slice(part * rows, (part + 1) * rows)
                here = stat_lane == heads * shelf + 2 * pair + part
                peaks = jnp.where(here, peak[own], peaks)
                totals = jnp.where(here, total[own], totals)
    count = CORES * heads
    high = totals.astype(bf16).astype(f32)
    low_part = pltpu.roll(totals - high, 2 * count, 1)
    stats = jnp.where(stat_lane < 2 * count, pltpu.roll(high, count, 1), low_part)
    stats = jnp.where(stat_lane < count, peaks, stats)
    both = jnp.concatenate(contexts + [stats.astype(bf16)], axis=1)
    out[...] = both.reshape(out.shape)
    w_copy.wait()


def merge_kernel(box, w_out, reads, out, got):
    chips, slots, wide = box.shape
    rows = chips * slots
    width = (wide - LANES) // CORES
    heads = width // DK
    requests = reads.shape[0]
    read = reads[...] > 0.0
    got[...] = box[...].reshape(rows, wide)
    stats = got[:, CORES * width :].astype(f32).T

    def stat(kind, h):
        at = kind * CORES * heads + h
        return jnp.concatenate([stats[at : at + 1], stats[at + heads : at + heads + 1]], axis=1)

    shares = []
    totals = []
    for h in range(heads):
        peak = jnp.where(read, stat(0, h), far_below)
        best = jnp.max(peak, axis=1, keepdims=True)
        total = stat(1, h) + stat(2, h)
        share = jnp.where(read, total * jnp.exp(peak - best), 0.0)
        shares.append(share)
        totals.append(jnp.sum(share, axis=1, keepdims=True))
    share = jnp.concatenate(shares, axis=0)
    high = share.astype(bf16)
    rest = (share - high.astype(f32)).astype(bf16)
    context = jnp.concatenate([got[:, :width], got[:, width : 2 * width]], axis=0)
    summed = dot(high, context, ((1,), (0,))) + dot(rest, context, ((1,), (0,)))
    head_of = lax.broadcasted_iota(jnp.int32, (requests, width), 1) // DK
    attended = jnp.zeros((requests, width), f32)
    for h in range(heads):
        part = summed[h * requests : (h + 1) * requests] / totals[h]
        attended = jnp.where(head_of == h, part, attended)
    attended = attended.astype(bf16)
    groups, _, columns = out.shape
    for n, g in enumerate(rotated(groups, groups // 2)):
        out[n] = dot(attended, w_out[:, g * columns : (g + 1) * columns], ((1,), (0,)))


def stage_kernel(shelf_ids, live_mask, keys, values, near_keys, near_values, reads, arrived):
    copies = [
        pltpu.make_async_copy(keys, near_keys, arrived.at[0]),
        pltpu.make_async_copy(values, near_values, arrived.at[1]),
    ]
    for copy in copies:
        copy.start()
    chips = reads.shape[1] // (CORES * SLOTS)
    _, live0, live1 = choose(shelf_ids[...], live_mask[...], chips, own_core())
    reads[...] = live0 + live1
    for copy in copies:
        copy.wait()


def in_vmem(shape, dtype):
    return pltpu.VMEM(shape, dtype)


def call(kernel, results, name, near, far=(), hbm=(), scratch=(), room=KERNEL_VMEM):
    spec = pl.BlockSpec(memory_space=pltpu.VMEM)
    near = [pltpu.with_memory_space_constraint(a, pltpu.VMEM) for a in near]
    far, hbm = [
        [pltpu.with_memory_space_constraint(a, pltpu.HBM) for a in some] for some in (far, hbm)
    ]
    return pl.pallas_call(
        kernel,
        out_shape=[in_vmem(*result) for result in results],
        in_specs=[spec] * (len(near) + len(far)) + [pl.BlockSpec(memory_space=pl.ANY)] * len(hbm),
        out_specs=[spec] * len(results),
        scratch_shapes=list(scratch),
        compiler_params=pltpu.CompilerParams(vmem_limit_bytes=room),
        name=name,
    )(*near, *far, *hbm)


def per_device(queries, passage_keys, passage_values, shelf_ids, live_mask, w_out):
    owners = lax.axis_size("psg")
    groups = lax.axis_size("head")
    requests, width = queries.shape

    def exchanged(x, axis, index_groups):
        return lax.all_to_all(
            x, axis, split_axis=0, concat_axis=0, axis_index_groups=index_groups, tiled=True
        )

    def from_other_core(x):
        return lax.ppermute(x, "psg", [(i, i ^ 1) for i in range(owners)])

    same_core = same_core_groups(owners)
    chips = owners // CORES
    wide = CORES * width + LANES
    box_array = ((chips, SLOTS, wide), bf16)
    rows = pltpu.VMEM((chips * SLOTS, wide), bf16)
    (box,) = call(box_kernel, [box_array], "box", (), (queries, shelf_ids, live_mask))
    keys, values, reads = call(
        stage_kernel,
        [
            (passage_keys.shape, bf16),
            (passage_values.shape, bf16),
            ((requests, CORES * SLOTS * chips), f32),
        ],
        "stage",
        (),
        (shelf_ids, live_mask),
        (passage_keys, passage_values),
        (pltpu.SemaphoreType.DMA((2,)),),
        2 << 20,
    )
    partials, w_near = call(
        shelf_kernel,
        [box_array, (w_out.shape, w_out.dtype)],
        "shelf",
        (
            exchanged(box, "psg", same_core),
            keys,
            values,
            from_other_core(passage_keys),
            from_other_core(passage_values),
        ),
        hbm=(w_out,),
        scratch=(rows, pltpu.SemaphoreType.DMA),
    )
    (projected,) = call(
        merge_kernel,
        [((groups, requests, w_out.shape[1] // groups), f32)],
        "merge",
        (exchanged(partials, "psg", same_core), w_near, reads),
        scratch=(rows,),
    )
    blocks = exchanged(projected, "head", [rotated(groups, groups // 2)])
    return jnp.sum(blocks, axis=0).astype(bf16)


def solution(mesh):
    in_specs = (
        P("psg", "head"),
        P("psg", None, "head"),
        P("psg", None, "head"),
        P("psg", None),
        P("psg", None),
        P("head", None),
    )
    out_specs = P("psg", "head")
    return jax.shard_map(
        per_device, mesh=mesh, in_specs=in_specs, out_specs=out_specs, check_vma=False
    )
```

```python
import jax
import jax.numpy as jnp
from jax import lax
from jax.experimental import pallas as pl
from jax.experimental.pallas import tpu as pltpu
from jax.sharding import PartitionSpec as P

DK = 64
SLOTS = 2
CORES = 2
LANES = 128
KERNEL_VMEM = 24 << 20
far_below = -1e30
bf16 = jnp.bfloat16
f32 = jnp.float32


def first_chip(chips):
    return chips * 45 // 64 if chips >= 32 else 0


def rotated(length, first):
    return [(first + i) % length for i in range(length)]


def same_core_groups(owners):
    chips = owners // CORES
    order = rotated(chips, first_chip(chips))
    return [[CORES * chip + core for chip in order] for core in range(CORES)]


def dot(a, b, dims):
    return lax.dot_general(a, b, (dims, ((), ())), preferred_element_type=f32)


def own_core():
    return lax.axis_index("psg") % CORES


def choose(shelf_ids, live_mask, chips, core):
    requests, shelves = shelf_ids.shape
    half = chips * SLOTS
    columns = CORES * half
    column = lax.broadcasted_iota(jnp.int32, (requests, columns), 1)
    other = (column >= half).astype(jnp.int32)
    place = (column - other * half) // SLOTS + first_chip(chips)
    chip = jnp.where(place >= chips, place - chips, place)
    owner = CORES * chip + jnp.where(other == core, 0, 1)
    present = jnp.zeros((requests, columns), f32)
    live0 = jnp.zeros((requests, columns), f32)
    live1 = jnp.zeros((requests, columns), f32)
    for j in range(shelves):
        hit = (shelf_ids[:, j : j + 1] == owner).astype(f32)
        present = present + hit
        first = live_mask[:, 2 * j : 2 * j + 1].astype(f32)
        first = jnp.ones_like(first) if j == 0 else first
        live0 = live0 + hit * first
        live1 = live1 + hit * live_mask[:, 2 * j + 1 : 2 * j + 2].astype(f32)
    rank = jnp.zeros((1, columns), f32)
    ranks = []
    for r in range(requests):
        ranks.append(rank)
        rank = rank + present[r : r + 1]
    rank = jnp.concatenate(ranks, axis=0)
    slot = (column % SLOTS).astype(f32)
    mine = jnp.where(rank == slot, present, 0.0)
    return mine, mine * live0, mine * live1


def box_kernel(queries, shelf_ids, live_mask, box, built, sent):
    requests, width = queries.shape
    chips = box.shape[0]
    half = chips * SLOTS
    mine, live0, live1 = choose(shelf_ids[...], live_mask[...], chips, own_core())
    dead0 = live1 * (1.0 - live0)
    dead1 = live0 * (1.0 - live1)
    dead = [dead0[:, :half], dead1[:, :half], dead0[:, half:], dead1[:, half:]]
    lane = lax.broadcasted_iota(jnp.int32, (requests, LANES), 1)
    rows = dot(mine.astype(bf16), queries[...], ((0,), (0,)))
    flags = dot(
        jnp.concatenate(dead, axis=0).astype(bf16),
        jnp.concatenate([(lane == n).astype(f32) for n in range(len(dead))], axis=0).astype(bf16),
        ((0,), (0,)),
    )
    pieces = sent.shape[0]
    part = chips // pieces
    copies = []
    for n in range(pieces):
        own = slice(n * part * SLOTS, (n + 1) * part * SLOTS)
        both = jnp.concatenate([rows[:half][own], rows[half:][own], flags[own]], axis=1)
        at = pl.ds(n * part, part)
        built[at] = both.astype(bf16).reshape(part, SLOTS, both.shape[1])
        copies.append(pltpu.make_async_copy(built.at[at], box.at[at], sent.at[n]))
        copies[-1].start()
    for copy in copies:
        copy.wait()


def shelf_kernel(box, keys, values, other_keys, other_values, w_out, out, w_near, got, arrived):
    w_copy = pltpu.make_async_copy(w_out, w_near, arrived)
    w_copy.start()
    chips, slots, wide = box.shape
    rows = chips * slots
    width = (wide - LANES) // CORES
    passages, length, _ = keys.shape
    positions = passages * length
    heads = width // DK
    got[...] = box[...].reshape(rows, wide)
    flags = got[:, CORES * width :]
    flags = jnp.concatenate([flags, flags], axis=0)
    place = lax.broadcasted_iota(jnp.int32, (positions, LANES), 0) // length
    lane = lax.broadcasted_iota(jnp.int32, (positions, LANES), 1)
    ones = jnp.ones((positions, LANES), bf16)
    stat_lane = lax.broadcasted_iota(jnp.int32, (rows, LANES), 1)
    low = stat_lane < DK
    keep = [jnp.where(low, 1.0, 0.0).astype(bf16), jnp.where(low, 0.0, 1.0).astype(bf16)]
    stats = jnp.zeros((rows, LANES), f32)
    contexts = []
    for shelf, (key_ref, value_ref) in enumerate(((keys, values), (other_keys, other_values))):
        bias = jnp.where(place + passages * shelf == lane, far_below, 0.0).astype(bf16)
        key_rows = key_ref[...].reshape(positions, width)
        value_rows = value_ref[...].reshape(positions, width)
        for pair in range(width // LANES):
            at = pair * LANES
            query_pair = got[:, shelf * width + at : shelf * width + at + LANES]
            query = jnp.concatenate([query_pair * keep[0], query_pair * keep[1]], axis=0)
            key_pair = jnp.concatenate([key_rows[:, at : at + LANES], bias], axis=1)
            value_pair = jnp.concatenate([value_rows[:, at : at + LANES], ones], axis=1)
            scores = dot(jnp.concatenate([query, flags], axis=1), key_pair, ((1,), (1,)))
            peak = jnp.max(scores, axis=1, keepdims=True).astype(bf16).astype(f32)
            weights = jnp.exp(scores - peak).astype(bf16)
            summed = dot(weights, value_pair, ((1,), (0,)))
            total = summed[:, LANES:]
            context = summed[:, :LANES] / total
            contexts.append(jnp.where(low, context[:rows], context[rows:]).astype(bf16))
            high = total.astype(bf16).astype(f32)
            for part in range(2):
                own = slice(part * rows, (part + 1) * rows)
                at_lane = 3 * heads * shelf + 2 * pair + part
                stats = jnp.where(stat_lane == at_lane, peak[own], stats)
                stats = jnp.where(stat_lane == at_lane + heads, high[own], stats)
                stats = jnp.where(stat_lane == at_lane + 2 * heads, (total - high)[own], stats)
    both = jnp.concatenate(contexts + [stats.astype(bf16)], axis=1)
    out[...] = both.reshape(out.shape)
    w_copy.wait()


def merge_kernel(box, w_out, shelf_ids, live_mask, out, got):
    chips, slots, wide = box.shape
    rows = chips * slots
    width = (wide - LANES) // CORES
    heads = width // DK
    requests = shelf_ids.shape[0]
    mine, live0, live1 = choose(shelf_ids[...], live_mask[...], chips, own_core())
    read = (live0 + live1) > 0.0
    got[...] = box[...].reshape(rows, wide)
    stats = got[:, CORES * width :].astype(f32).T

    def stat(n):
        return jnp.concatenate([stats[n : n + 1], stats[3 * heads + n : 3 * heads + n + 1]], axis=1)

    shares = []
    totals = []
    for h in range(heads):
        peak = jnp.where(read, stat(h), far_below)
        best = jnp.max(peak, axis=1, keepdims=True)
        total = stat(heads + h) + stat(2 * heads + h)
        share = jnp.where(read, total * jnp.exp(peak - best), 0.0)
        shares.append(share)
        totals.append(jnp.sum(share, axis=1, keepdims=True))
    share = jnp.concatenate(shares, axis=0)
    high = share.astype(bf16)
    rest = (share - high.astype(f32)).astype(bf16)
    context = jnp.concatenate([got[:, :width], got[:, width : 2 * width]], axis=0)
    summed = dot(high, context, ((1,), (0,))) + dot(rest, context, ((1,), (0,)))
    head_of = lax.broadcasted_iota(jnp.int32, (requests, width), 1) // DK
    attended = jnp.zeros((requests, width), f32)
    for h in range(heads):
        part = summed[h * requests : (h + 1) * requests] / totals[h]
        attended = jnp.where(head_of == h, part, attended)
    attended = attended.astype(bf16)
    groups, _, columns = out.shape
    for n, g in enumerate(rotated(groups, groups // 4)):
        out[n] = dot(attended, w_out[:, g * columns : (g + 1) * columns], ((1,), (0,)))


def stage_kernel(*refs):
    count = (len(refs) - 1) // 2
    copies = [
        pltpu.make_async_copy(
            refs[n].at[tuple(pl.ds(0, k) for k in refs[count + n].shape)],
            refs[count + n],
            refs[-1].at[n],
        )
        for n in range(count)
    ]
    for copy in copies:
        copy.start()
    for copy in copies:
        copy.wait()


def in_vmem(shape, dtype):
    return pltpu.VMEM(shape, dtype)


def staged(*arrays):
    return pl.pallas_call(
        stage_kernel,
        out_shape=[in_vmem(a.shape, a.dtype) for a in arrays],
        in_specs=[pl.BlockSpec(memory_space=pl.ANY)] * len(arrays),
        out_specs=[pl.BlockSpec(memory_space=pltpu.VMEM)] * len(arrays),
        scratch_shapes=[pltpu.SemaphoreType.DMA((len(arrays),))],
        compiler_params=pltpu.CompilerParams(vmem_limit_bytes=1 << 20),
        name="stage",
    )(*[pltpu.with_memory_space_constraint(a, pltpu.HBM) for a in arrays])


def call(kernel, results, name, near, far=(), hbm=(), scratch=()):
    spec = pl.BlockSpec(memory_space=pltpu.VMEM)
    near = [pltpu.with_memory_space_constraint(a, pltpu.VMEM) for a in near]
    far, hbm = [
        [pltpu.with_memory_space_constraint(a, pltpu.HBM) for a in some] for some in (far, hbm)
    ]
    return pl.pallas_call(
        kernel,
        out_shape=[in_vmem(*result) for result in results],
        in_specs=[spec] * (len(near) + len(far)) + [pl.BlockSpec(memory_space=pl.ANY)] * len(hbm),
        out_specs=[spec] * len(results),
        scratch_shapes=list(scratch),
        compiler_params=pltpu.CompilerParams(vmem_limit_bytes=KERNEL_VMEM),
        name=name,
    )(*near, *far, *hbm)


def per_device(queries, passage_keys, passage_values, shelf_ids, live_mask, w_out):
    owners = lax.axis_size("psg")
    groups = lax.axis_size("head")
    requests, width = queries.shape

    def exchanged(x, axis, index_groups):
        return lax.all_to_all(
            x, axis, split_axis=0, concat_axis=0, axis_index_groups=index_groups, tiled=True
        )

    def from_other_core(x):
        return lax.ppermute(x, "psg", [(i, i ^ 1) for i in range(owners)])

    same_core = same_core_groups(owners)
    chips = owners // CORES
    wide = CORES * width + LANES
    box_array = ((chips, SLOTS, wide), bf16)
    rows = pltpu.VMEM((chips * SLOTS, wide), bf16)
    box = pl.pallas_call(
        box_kernel,
        out_shape=jax.ShapeDtypeStruct(*box_array),
        in_specs=[pl.BlockSpec(memory_space=pltpu.VMEM)] * 3,
        out_specs=pl.BlockSpec(memory_space=pl.ANY),
        scratch_shapes=[pltpu.VMEM(*box_array), pltpu.SemaphoreType.DMA((4,))],
        compiler_params=pltpu.CompilerParams(vmem_limit_bytes=4 << 20),
        name="box",
    )(*[pltpu.with_memory_space_constraint(a, pltpu.HBM) for a in (queries, shelf_ids, live_mask)])
    keys, values, ids_near, live_near = staged(passage_keys, passage_values, shelf_ids, live_mask)
    partials, w_near = call(
        shelf_kernel,
        [box_array, (w_out.shape, w_out.dtype)],
        "shelf",
        (
            exchanged(box, "psg", same_core),
            keys,
            values,
            from_other_core(passage_keys),
            from_other_core(passage_values),
        ),
        hbm=(w_out,),
        scratch=(rows, pltpu.SemaphoreType.DMA),
    )
    (projected,) = call(
        merge_kernel,
        [((groups, requests, w_out.shape[1] // groups), f32)],
        "merge",
        (exchanged(partials, "psg", same_core), w_near, ids_near, live_near),
        scratch=(rows,),
    )
    blocks = exchanged(projected, "head", [rotated(groups, groups // 4)])
    return jnp.sum(blocks, axis=0).astype(bf16)


def solution(mesh):
    in_specs = (
        P("psg", "head"),
        P("psg", None, "head"),
        P("psg", None, "head"),
        P("psg", None),
        P("psg", None),
        P("head", None),
    )
    out_specs = P("psg", "head")
    return jax.shard_map(
        per_device, mesh=mesh, in_specs=in_specs, out_specs=out_specs, check_vma=False
    )
```

```python
import jax
import jax.numpy as jnp
from jax import lax
from jax.experimental import pallas as pl
from jax.experimental.pallas import tpu as pltpu
from jax.sharding import PartitionSpec as P

DK = 64
SLOTS = 2
CORES = 2
LANES = 128
KERNEL_VMEM = 24 << 20
far_below = -1e30
bf16 = jnp.bfloat16
f32 = jnp.float32


def first_chip(chips):
    return chips * 45 // 64 if chips >= 32 else 0


def rotated(length, first):
    return [(first + i) % length for i in range(length)]


def same_core_groups(owners):
    chips = owners // CORES
    order = rotated(chips, first_chip(chips))
    return [[CORES * chip + core for chip in order] for core in range(CORES)]


def dot(a, b, dims):
    return lax.dot_general(a, b, (dims, ((), ())), preferred_element_type=f32)


def own_core():
    return lax.axis_index("psg") % CORES


def choose(shelf_ids, live_mask, chips, core):
    requests, shelves = shelf_ids.shape
    half = chips * SLOTS
    columns = CORES * half
    column = lax.broadcasted_iota(jnp.int32, (requests, columns), 1)
    other = (column >= half).astype(jnp.int32)
    place = (column - other * half) // SLOTS + first_chip(chips)
    chip = jnp.where(place >= chips, place - chips, place)
    owner = CORES * chip + jnp.where(other == core, 0, 1)
    present = jnp.zeros((requests, columns), f32)
    live0 = jnp.zeros((requests, columns), f32)
    live1 = jnp.zeros((requests, columns), f32)
    for j in range(shelves):
        hit = (shelf_ids[:, j : j + 1] == owner).astype(f32)
        present = present + hit
        first = live_mask[:, 2 * j : 2 * j + 1].astype(f32)
        first = jnp.ones_like(first) if j == 0 else first
        live0 = live0 + hit * first
        live1 = live1 + hit * live_mask[:, 2 * j + 1 : 2 * j + 2].astype(f32)
    rank = jnp.zeros((1, columns), f32)
    ranks = []
    for r in range(requests):
        ranks.append(rank)
        rank = rank + present[r : r + 1]
    rank = jnp.concatenate(ranks, axis=0)
    slot = (column % SLOTS).astype(f32)
    mine = jnp.where(rank == slot, present, 0.0)
    return mine, mine * live0, mine * live1


def box_kernel(queries, shelf_ids, live_mask, box, built, sent):
    requests, width = queries.shape
    chips = box.shape[0]
    half = chips * SLOTS
    mine, live0, live1 = choose(shelf_ids[...], live_mask[...], chips, own_core())
    dead0 = live1 * (1.0 - live0)
    dead1 = live0 * (1.0 - live1)
    dead = [dead0[:, :half], dead1[:, :half], dead0[:, half:], dead1[:, half:]]
    lane = lax.broadcasted_iota(jnp.int32, (requests, LANES), 1)
    rows = dot(mine.astype(bf16), queries[...], ((0,), (0,)))
    flags = dot(
        jnp.concatenate(dead, axis=0).astype(bf16),
        jnp.concatenate([(lane == n).astype(f32) for n in range(len(dead))], axis=0).astype(bf16),
        ((0,), (0,)),
    )
    pieces = sent.shape[0]
    part = chips // pieces
    copies = []
    for n in range(pieces):
        own = slice(n * part * SLOTS, (n + 1) * part * SLOTS)
        both = jnp.concatenate([rows[:half][own], rows[half:][own], flags[own]], axis=1)
        at = pl.ds(n * part, part)
        built[at] = both.astype(bf16).reshape(part, SLOTS, both.shape[1])
        copies.append(pltpu.make_async_copy(built.at[at], box.at[at], sent.at[n]))
        copies[-1].start()
    for copy in copies:
        copy.wait()


def shelf_kernel(box, keys, values, other_keys, other_values, w_out, out, w_near, got, arrived):
    w_copy = pltpu.make_async_copy(w_out, w_near, arrived)
    w_copy.start()
    chips, slots, wide = box.shape
    rows = chips * slots
    width = (wide - LANES) // CORES
    passages, length, _ = keys.shape
    positions = passages * length
    heads = width // DK
    got[...] = box[...].reshape(rows, wide)
    flags = got[:, CORES * width :]
    flags = jnp.concatenate([flags, flags], axis=0)
    place = lax.broadcasted_iota(jnp.int32, (positions, LANES), 0) // length
    lane = lax.broadcasted_iota(jnp.int32, (positions, LANES), 1)
    ones = jnp.ones((positions, LANES), bf16)
    stat_lane = lax.broadcasted_iota(jnp.int32, (rows, LANES), 1)
    low = stat_lane < DK
    keep = [jnp.where(low, 1.0, 0.0).astype(bf16), jnp.where(low, 0.0, 1.0).astype(bf16)]
    stats = jnp.zeros((rows, LANES), f32)
    contexts = []
    for shelf, (key_ref, value_ref) in enumerate(((keys, values), (other_keys, other_values))):
        bias = jnp.where(place + passages * shelf == lane, far_below, 0.0).astype(bf16)
        key_rows = key_ref[...].reshape(positions, width)
        value_rows = value_ref[...].reshape(positions, width)
        for pair in range(width // LANES):
            at = pair * LANES
            query_pair = got[:, shelf * width + at : shelf * width + at + LANES]
            query = jnp.concatenate([query_pair * keep[0], query_pair * keep[1]], axis=0)
            key_pair = jnp.concatenate([key_rows[:, at : at + LANES], bias], axis=1)
            value_pair = jnp.concatenate([value_rows[:, at : at + LANES], ones], axis=1)
            scores = dot(jnp.concatenate([query, flags], axis=1), key_pair, ((1,), (1,)))
            peak = jnp.max(scores, axis=1, keepdims=True).astype(bf16).astype(f32)
            weights = jnp.exp(scores - peak).astype(bf16)
            summed = dot(weights, value_pair, ((1,), (0,)))
            total = summed[:, LANES:]
            context = summed[:, :LANES] / total
            contexts.append(jnp.where(low, context[:rows], context[rows:]).astype(bf16))
            high = total.astype(bf16).astype(f32)
            for part in range(2):
                own = slice(part * rows, (part + 1) * rows)
                at_lane = 3 * heads * shelf + 2 * pair + part
                stats = jnp.where(stat_lane == at_lane, peak[own], stats)
                stats = jnp.where(stat_lane == at_lane + heads, high[own], stats)
                stats = jnp.where(stat_lane == at_lane + 2 * heads, (total - high)[own], stats)
    both = jnp.concatenate(contexts + [stats.astype(bf16)], axis=1)
    out[...] = both.reshape(out.shape)
    w_copy.wait()


def merge_kernel(box, w_out, shelf_ids, live_mask, out, got):
    chips, slots, wide = box.shape
    rows = chips * slots
    width = (wide - LANES) // CORES
    heads = width // DK
    requests = shelf_ids.shape[0]
    mine, live0, live1 = choose(shelf_ids[...], live_mask[...], chips, own_core())
    read = (live0 + live1) > 0.0
    got[...] = box[...].reshape(rows, wide)
    stats = got[:, CORES * width :].astype(f32).T

    def stat(n):
        return jnp.concatenate([stats[n : n + 1], stats[3 * heads + n : 3 * heads + n + 1]], axis=1)

    shares = []
    totals = []
    for h in range(heads):
        peak = jnp.where(read, stat(h), far_below)
        best = jnp.max(peak, axis=1, keepdims=True)
        total = stat(heads + h) + stat(2 * heads + h)
        share = jnp.where(read, total * jnp.exp(peak - best), 0.0)
        shares.append(share)
        totals.append(jnp.sum(share, axis=1, keepdims=True))
    share = jnp.concatenate(shares, axis=0)
    high = share.astype(bf16)
    rest = (share - high.astype(f32)).astype(bf16)
    context = jnp.concatenate([got[:, :width], got[:, width : 2 * width]], axis=0)
    summed = dot(high, context, ((1,), (0,))) + dot(rest, context, ((1,), (0,)))
    head_of = lax.broadcasted_iota(jnp.int32, (requests, width), 1) // DK
    attended = jnp.zeros((requests, width), f32)
    for h in range(heads):
        part = summed[h * requests : (h + 1) * requests] / totals[h]
        attended = jnp.where(head_of == h, part, attended)
    attended = attended.astype(bf16)
    groups, _, columns = out.shape
    for n, g in enumerate(rotated(groups, groups // 2)):
        out[n] = dot(attended, w_out[:, g * columns : (g + 1) * columns], ((1,), (0,)))


def stage_kernel(*refs):
    count = (len(refs) - 1) // 2
    copies = [
        pltpu.make_async_copy(
            refs[n].at[tuple(pl.ds(0, k) for k in refs[count + n].shape)],
            refs[count + n],
            refs[-1].at[n],
        )
        for n in range(count)
    ]
    for copy in copies:
        copy.start()
    for copy in copies:
        copy.wait()


def in_vmem(shape, dtype):
    return pltpu.VMEM(shape, dtype)


def staged(*arrays):
    return pl.pallas_call(
        stage_kernel,
        out_shape=[in_vmem(a.shape, a.dtype) for a in arrays],
        in_specs=[pl.BlockSpec(memory_space=pl.ANY)] * len(arrays),
        out_specs=[pl.BlockSpec(memory_space=pltpu.VMEM)] * len(arrays),
        scratch_shapes=[pltpu.SemaphoreType.DMA((len(arrays),))],
        compiler_params=pltpu.CompilerParams(vmem_limit_bytes=1 << 20),
        name="stage",
    )(*[pltpu.with_memory_space_constraint(a, pltpu.HBM) for a in arrays])


def call(kernel, results, name, near, far=(), hbm=(), scratch=()):
    spec = pl.BlockSpec(memory_space=pltpu.VMEM)
    near = [pltpu.with_memory_space_constraint(a, pltpu.VMEM) for a in near]
    far, hbm = [
        [pltpu.with_memory_space_constraint(a, pltpu.HBM) for a in some] for some in (far, hbm)
    ]
    return pl.pallas_call(
        kernel,
        out_shape=[in_vmem(*result) for result in results],
        in_specs=[spec] * (len(near) + len(far)) + [pl.BlockSpec(memory_space=pl.ANY)] * len(hbm),
        out_specs=[spec] * len(results),
        scratch_shapes=list(scratch),
        compiler_params=pltpu.CompilerParams(vmem_limit_bytes=KERNEL_VMEM),
        name=name,
    )(*near, *far, *hbm)


def per_device(queries, passage_keys, passage_values, shelf_ids, live_mask, w_out):
    owners = lax.axis_size("psg")
    groups = lax.axis_size("head")
    requests, width = queries.shape

    def exchanged(x, axis, index_groups):
        return lax.all_to_all(
            x, axis, split_axis=0, concat_axis=0, axis_index_groups=index_groups, tiled=True
        )

    def from_other_core(x):
        return lax.ppermute(x, "psg", [(i, i ^ 1) for i in range(owners)])

    same_core = same_core_groups(owners)
    chips = owners // CORES
    wide = CORES * width + LANES
    box_array = ((chips, SLOTS, wide), bf16)
    rows = pltpu.VMEM((chips * SLOTS, wide), bf16)
    box = pl.pallas_call(
        box_kernel,
        out_shape=jax.ShapeDtypeStruct(*box_array),
        in_specs=[pl.BlockSpec(memory_space=pltpu.VMEM)] * 3,
        out_specs=pl.BlockSpec(memory_space=pl.ANY),
        scratch_shapes=[pltpu.VMEM(*box_array), pltpu.SemaphoreType.DMA((4,))],
        compiler_params=pltpu.CompilerParams(vmem_limit_bytes=4 << 20),
        name="box",
    )(*[pltpu.with_memory_space_constraint(a, pltpu.HBM) for a in (queries, shelf_ids, live_mask)])
    keys, values, ids_near, live_near = staged(passage_keys, passage_values, shelf_ids, live_mask)
    partials, w_near = call(
        shelf_kernel,
        [box_array, (w_out.shape, w_out.dtype)],
        "shelf",
        (
            exchanged(box, "psg", same_core),
            keys,
            values,
            from_other_core(passage_keys),
            from_other_core(passage_values),
        ),
        hbm=(w_out,),
        scratch=(rows, pltpu.SemaphoreType.DMA),
    )
    (projected,) = call(
        merge_kernel,
        [((groups, requests, w_out.shape[1] // groups), f32)],
        "merge",
        (exchanged(partials, "psg", same_core), w_near, ids_near, live_near),
        scratch=(rows,),
    )
    blocks = exchanged(projected, "head", [rotated(groups, groups // 2)])
    return jnp.sum(blocks, axis=0).astype(bf16)


def solution(mesh):
    in_specs = (
        P("psg", "head"),
        P("psg", None, "head"),
        P("psg", None, "head"),
        P("psg", None),
        P("psg", None),
        P("head", None),
    )
    out_specs = P("psg", "head")
    return jax.shard_map(
        per_device, mesh=mesh, in_specs=in_specs, out_specs=out_specs, check_vma=False
    )
```
